512 devices in a mesh: hap: 8 (over x, y_lo), snp: 64 (over z, y_hi, core).
Axes of the slice: x: 4, y: 4 (y_hi: 2, y_lo: 2; y = y_hi * 2 + y_lo), z: 16, core: 2. Of those that a mesh axis runs over, the one named last changes fastest.
Arguments:
- packed_panel: int32 [384, 65536], P('hap', 'snp'), may hold values from 0 to 8191, as said below
- components: bfloat16 [64, 4992], P(None, 'hap'), may hold values from -0.078125 to 0.078125
- bounds: int32 [2, 65536], P(None, 'snp'), may hold values from 0 to 65535, as said below
- band_width: int32 [65536], P('snp'), may hold values from 1 to 256
Outputs:
- ld_scores: float32 [65536], P('snp')
The draws below stay inside these ranges and needn't reach their ends.
Inputs may be any that keep to these rules, and one draw needn't show every extreme that they name: Bit j of packed_panel[w, s] (j from 0 to 12) is the allele of haplotype 13 w + j at SNP s; higher bits are zero. LD blocks are consecutive runs of 1 to 2048 SNPs that cover all SNPs in order; bounds[0, s] and bounds[1, s] are the first and last SNP of the block holding s.
All inputs are finite; a program needn't handle non-finite values.
Results may differ from the reference program's by a relative error of at most 0.00074.
Values may be sent and summed in bfloat16 or wider, within the bound.
A program may use at most 64 MiB of HBM per device.

```python
import jax
import jax.numpy as jnp
from jax import lax

K = 64
SNP_DEV = 1024
HAPS = 4992
SNPS = 65536
BAND = 256
BLOCK_MOST = 2048
N_SNP = 64


def draw_packed_panel(key, part):
    positions = jnp.arange(SNPS, dtype=jnp.int32)
    trend = 100 + 600 * positions // SNPS
    jitter = jax.random.randint(jax.random.fold_in(key, 1), (SNPS,), -80, 81, dtype=jnp.int32)
    frequency = trend + jitter
    shifts = jnp.arange(13, dtype=jnp.int32)
    row_key = jax.random.fold_in(key, 2)

    def word_row(row_index):
        draws = jax.random.randint(jax.random.fold_in(row_key, row_index), (13, SNPS), 0, 1000, dtype=jnp.int32)
        bit_values = (draws < frequency[None, :]).astype(jnp.int32)
        return jnp.sum(jnp.left_shift(bit_values, shifts[:, None]), axis=0).astype(jnp.int32)
    return lax.map(word_row, jnp.arange(HAPS // 13, dtype=jnp.int32))


def draw_bounds(key, part):
    lengths = jax.random.randint(jax.random.fold_in(key, 3), (SNPS,), 2, BLOCK_MOST + 1, dtype=jnp.int32)
    single = jax.random.randint(jax.random.fold_in(key, 4), (SNPS,), 0, 8, dtype=jnp.int32)
    lengths = jnp.where(single == 0, 1, lengths)
    widest = jax.random.randint(jax.random.fold_in(key, 5), (), 0, 8, dtype=jnp.int32)
    positions = jnp.arange(SNPS, dtype=jnp.int32)
    lengths = jnp.where(positions == widest, BLOCK_MOST, lengths).astype(jnp.int32)
    block_ends = jnp.cumsum(lengths).astype(jnp.int32)
    block_index = jnp.searchsorted(block_ends, positions, side='right').astype(jnp.int32)
    block_first = block_ends[block_index] - lengths[block_index]
    block_last = jnp.minimum(block_ends[block_index] - 1, SNPS - 1)
    return jnp.stack([block_first, block_last]).astype(jnp.int32)


def place_ends(drawn, key, smallest, largest):
    place = [jax.random.randint(jax.random.fold_in(key, axis), (), 0, length) for axis, length in enumerate(drawn.shape)]
    main_axis = drawn.shape.index(max(drawn.shape))
    neighbour = place[:main_axis] + [(place[main_axis] + 1) % drawn.shape[main_axis]] + place[main_axis + 1:]
    return drawn.at[tuple(place)].set(smallest).at[tuple(neighbour)].set(largest)


def level_of(own_key, dims, pieces, least, largest):
    gain, own = 1.0, jax.random.fold_in(own_key, 6)
    for axis_at, parts in pieces:
        heights = jnp.exp(jax.random.uniform(jax.random.fold_in(own, axis_at), (parts,), jnp.float32, least / len(pieces), largest / len(pieces)))
        gain = gain * jnp.repeat(heights, dims[axis_at] // parts).reshape([-1 if axis == axis_at else 1 for axis in range(len(dims))])
    return gain


def scatter_about(rng, dims, deviation, reach, split=(), kind=jnp.bfloat16):
    values = jax.random.normal(rng, dims, jnp.float32) * deviation
    if len(split) > 0:
        values = level_of(rng, dims, split, -0.22, 0.18) * values
    return jnp.clip(values, min=-reach, max=reach).astype(kind)


def setup_inputs(seed: int = 0) -> dict:
    splits = jax.random.split(jax.random.key(seed), 5)
    packed_panel = draw_packed_panel(jax.random.fold_in(splits[4], 71), 0)
    components = scatter_about(splits[1], (K, HAPS), HAPS ** -0.5, 0.078125, ((1, 8),))
    bounds = draw_bounds(jax.random.fold_in(splits[4], 71), 0)
    band_width = place_ends(jax.random.randint(splits[3], (SNPS,), 1, BAND + 1), jax.random.fold_in(splits[3], 1), 1, BAND).astype(jnp.int32)
    return {"packed_panel": packed_panel, "components": components, "bounds": bounds, "band_width": band_width}


epsilon = 1e-06

def unpack(packed):
    shifts = jnp.arange(13, dtype=jnp.int32)
    bit_values = jnp.bitwise_and(jnp.right_shift(packed[:, None, :], shifts[None, :, None]), 1)
    return bit_values.reshape(packed.shape[0] * 13, packed.shape[1]).astype(jnp.bfloat16)

def standardize(factor):
    average = lax.optimization_barrier(jnp.mean(factor, axis=1, keepdims=True))
    centered = factor - average
    variance = lax.optimization_barrier(jnp.mean(centered * centered, axis=1, keepdims=True))
    return (centered * lax.rsqrt(variance + epsilon)).astype(jnp.bfloat16)

def band_scores(padded, inverse, bounds, band_width, offset, start_row, row_count, reach_width):
    component_count = padded.shape[0]
    block_size = min(256, row_count)

    def block_scores(block_index):
        first_row = start_row + block_index * block_size
        row_part = lax.dynamic_slice_in_dim(padded, first_row + reach_width, block_size, 1)
        column_part = lax.dynamic_slice_in_dim(padded, first_row, block_size + 2 * reach_width, 1)
        inverse_rows = lax.dynamic_slice_in_dim(inverse, first_row + reach_width, block_size, 0)
        inverse_columns = lax.dynamic_slice_in_dim(inverse, first_row, block_size + 2 * reach_width, 0)
        block_first = lax.dynamic_slice_in_dim(bounds[0], first_row, block_size, 0)
        block_last = lax.dynamic_slice_in_dim(bounds[1], first_row, block_size, 0)
        row_reach = lax.dynamic_slice_in_dim(band_width, first_row, block_size, 0)
        inner_products = lax.dot_general(row_part, column_part, (((0,), (0,)), ((), ())), preferred_element_type=jnp.float32)
        correlation = inner_products * (1.0 / component_count) * inverse_rows[:, None] * inverse_columns[None, :]
        row_position = offset + first_row + jnp.arange(block_size, dtype=jnp.int32)
        column_position = offset + first_row - reach_width + jnp.arange(block_size + 2 * reach_width, dtype=jnp.int32)
        window_low = jnp.maximum(block_first, row_position - row_reach)
        window_high = jnp.minimum(block_last, row_position + row_reach)
        inside = (column_position[None, :] >= window_low[:, None]) & (column_position[None, :] <= window_high[:, None]) & (column_position[None, :] != row_position[:, None])
        squared_sum = lax.optimization_barrier(jnp.sum(jnp.where(inside, correlation * correlation, 0.0), axis=1))
        window_count = lax.optimization_barrier(jnp.sum(inside.astype(jnp.float32), axis=1))
        return component_count * squared_sum / jnp.maximum(window_count, 1.0)
    blocks = jnp.arange(row_count // block_size, dtype=jnp.int32)
    return lax.map(block_scores, blocks).reshape(row_count)

def inverse_norms(padded):
    squares = jnp.square(padded.astype(jnp.float32))
    return lax.rsqrt(lax.optimization_barrier(jnp.mean(squares, axis=0)) + epsilon)

def reference(packed_panel, components, bounds, band_width):
    groups = packed_panel.reshape(packed_panel.shape[0], N_SNP, SNP_DEV).transpose(1, 0, 2)

    def project(packed):
        return jnp.dot(components, unpack(packed), preferred_element_type=jnp.float32)
    factor = lax.map(project, groups).transpose(1, 0, 2).reshape(components.shape[0], SNPS)
    normed = standardize(factor)
    padded = jnp.pad(normed, ((0, 0), (BAND, BAND)))
    inverse = inverse_norms(padded)
    return band_scores(padded, inverse, bounds, band_width, jnp.int32(0), 0, SNPS, BAND)
```

```python
import functools

import jax
import jax.numpy as jnp
from jax import lax
from jax.experimental import pallas as pl
from jax.experimental.pallas import tpu as pltpu
from jax.sharding import PartitionSpec as P

EPS = 1e-06
K = 64
BITS = 13
PIECE = 128
REACH = 2
WINDOW = 2 * REACH + 1
PLANE = 4
MESH = pl.DeviceIdType.MESH


def ring(value, size):
    return lax.rem(value, size)


def kernel(
    haps, snps, panel, comp, bounds, width, out,
    comp_pad, part, recv, full, normed, weight, masks, scale, near, far,
    part_send, part_recv, full_send, full_recv, halo_send, halo_recv,
    near_send, near_recv, far_send, far_recv,
):
    h, s = lax.axis_index("hap"), lax.axis_index("snp")
    z, sub = lax.div(s, PLANE), lax.rem(s, PLANE)
    planes, plane_size = snps // PLANE, haps * PLANE
    me = h * PLANE + sub
    words, columns = panel.shape
    pieces = columns // PIECE
    left, right = ring(s + snps - 1, snps), ring(s + 1, snps)

    def in_plane(r):
        q = ring(me + r, plane_size)
        return (lax.div(q, PLANE), z * PLANE + lax.rem(q, PLANE))

    def along_z(r):
        return (h, ring(z + r, planes) * PLANE + sub)

    barrier = pltpu.get_barrier_semaphore()

    def greet(device):
        pl.semaphore_signal(barrier, inc=1, device_id=device, device_id_type=MESH)

    @pl.loop(1, plane_size)
    def _(r):
        greet(in_plane(r))

    @pl.loop(1, planes)
    def _(r):
        greet(along_z(r))

    greet((h, left))
    greet((h, right))

    depth = comp_pad.shape[1]
    comp_pad[...] = jnp.zeros_like(comp_pad)
    comp_pad[:, : comp.shape[1]] = comp[...]
    col = lax.broadcasted_iota(jnp.int32, (8, depth), 1)
    bit = jnp.zeros_like(col)
    for j in range(1, BITS + 1):
        bit = bit + (col >= j * words).astype(jnp.int32)
    source = jnp.where(col < words * BITS, BITS * (col - words * bit) + bit, -1)[:1]
    level = (jnp.right_shift(1 << (BITS - 1), bit).astype(jnp.float32) * (0.5 ** (BITS - 1)))[:1]
    row = lax.broadcasted_iota(jnp.int32, (depth, depth), 0)
    chosen = jnp.where(row == source, level, 0.0).astype(jnp.bfloat16)
    mixed = jnp.dot(comp_pad[...], chosen, preferred_element_type=jnp.float32).astype(jnp.bfloat16)

    def project(block):
        at = pl.multiple_of(block * (2 * PIECE), 2 * PIECE)
        packed = panel[:, pl.ds(at, 2 * PIECE)]
        alleles = [
            jnp.bitwise_and(packed, 1 << j).astype(jnp.float32).astype(jnp.bfloat16)
            for j in range(BITS)
        ]
        rest = depth - BITS * words
        alleles.append(jnp.zeros((rest, 2 * PIECE), jnp.bfloat16))
        product = jnp.dot(
            mixed, jnp.concatenate(alleles, axis=0), preferred_element_type=jnp.float32
        )
        part[2 * block] = product[:, :PIECE]
        part[2 * block + 1] = product[:, PIECE:]

    def send_part(to):
        return pltpu.make_async_remote_copy(
            part.at[to], recv.at[h], part_send, part_recv, device_id=(to, s), device_id_type=MESH
        )

    blocks = pieces // 2
    mine, side = lax.div(h, 2), lax.rem(h, 2)
    order = sorted(range(blocks), key=lambda d: (-min(d, blocks - d), d))
    for turn, d in enumerate(order):
        block = ring(mine + d, blocks)
        project(block)
        if turn == 0:
            pl.semaphore_wait(barrier, plane_size + planes)
        if d:
            send_part(2 * block + side).start()
            send_part(2 * block + 1 - side).start()
        else:
            send_part(2 * block + 1 - side).start()
    recv[h] = part[h]

    def wait_for(ref, sem):
        pltpu.make_async_copy(ref, ref, sem).wait()

    wait_for(recv.at[pl.ds(0, pieces - 1)], part_recv)
    total = recv[0]
    for k in range(1, pieces):
        total = total + recv[k]
    full[REACH + h] = total

    lane = lax.broadcasted_iota(jnp.int32, (1, 2 * K), 1)
    first = lane < K
    both = jnp.concatenate([total, total], axis=0).T
    average = jnp.sum(both, axis=0, keepdims=True) * (1.0 / PIECE)
    off = both - average
    spread = jnp.sum(off * off, axis=0, keepdims=True)
    near[me] = jnp.where(first, average, spread)

    def send_near(r):
        return pltpu.make_async_remote_copy(
            near.at[me], near.at[me], near_send, near_recv,
            device_id=in_plane(r), device_id_type=MESH,
        )

    @pl.loop(1, plane_size)
    def _(r):
        send_near(r).start()

    def send_full(r):
        to = ring(h + r, haps)
        return pltpu.make_async_remote_copy(
            full.at[REACH + h], full.at[REACH + h], full_send, full_recv,
            device_id=(to, s), device_id_type=MESH,
        )

    for r in range(1, haps):
        send_full(r).start()

    def merge(ref, count, weight_each):
        rows = [ref[k] for k in range(count)]
        summed = functools.reduce(jnp.add, rows)
        mean = summed * (1.0 / count)
        offs = [r - mean for r in rows]
        between = functools.reduce(jnp.add, [o * o for o in offs]) * weight_each
        return mean, summed, between

    position = lax.broadcasted_iota(jnp.int32, (1, PIECE), 1)
    lane_at = lax.broadcasted_iota(jnp.int32, (PIECE, PIECE), 1)
    row_at = lax.broadcasted_iota(jnp.int32, (PIECE, PIECE), 0)

    def windows(b):
        at = s * columns + b * PIECE
        here = position + at
        reach = width[b : b + 1, :]
        cut = slice(b * PIECE, (b + 1) * PIECE)
        low = jnp.maximum(bounds[0:1, cut], here - reach)
        high = jnp.minimum(bounds[1:2, cut], here + reach)
        count = (high - low).astype(jnp.float32)
        scale[b : b + 1, :] = (1.0 / K) / jnp.maximum(count, 1.0)
        start = at - REACH * PIECE
        low_rows = jnp.broadcast_to((low - start).astype(jnp.float32), (PIECE, PIECE)).T
        high_rows = jnp.broadcast_to((high - start).astype(jnp.float32), (PIECE, PIECE)).T
        for t in range(WINDOW):
            there = (lane_at + t * PIECE).astype(jnp.float32)
            inside = (there >= low_rows) & (there <= high_rows)
            if t == REACH:
                inside = inside & (lane_at != row_at)
            masks[b, :, t * PIECE : (t + 1) * PIECE] = inside.astype(jnp.float32)

    for b in range(pieces):
        windows(b)

    wait_for(near.at[pl.ds(0, plane_size - 1)], near_recv)
    mean, summed, between = merge(near, plane_size, float(PIECE))
    moved = pltpu.roll(jnp.broadcast_to(between, (8, 2 * K)), K, 1)[:1]
    far[z] = jnp.where(first, mean, summed + moved)

    def send_far(r):
        return pltpu.make_async_remote_copy(
            far.at[z], far.at[z], far_send, far_recv, device_id=along_z(r), device_id_type=MESH
        )

    @pl.loop(1, planes)
    def _(r):
        send_far(r).start()

    wait_for(full.at[pl.ds(REACH, haps - 1)], full_recv)
    low_halo = pltpu.make_async_remote_copy(
        full.at[pl.ds(pieces, REACH)], full.at[pl.ds(0, REACH)],
        halo_send.at[0], halo_recv.at[0], device_id=(h, right), device_id_type=MESH,
    )
    high_halo = pltpu.make_async_remote_copy(
        full.at[pl.ds(REACH, REACH)], full.at[pl.ds(REACH + pieces, REACH)],
        halo_send.at[1], halo_recv.at[1], device_id=(h, left), device_id_type=MESH,
    )
    low_halo.start()
    high_halo.start()
    low_halo.wait_recv()
    high_halo.wait_recv()

    wait_for(far.at[pl.ds(0, planes - 1)], far_recv)
    mean, summed, between = merge(far, planes, float(PIECE * plane_size))
    top = jnp.broadcast_to(jnp.where(first, mean, summed), (2 * K, 2 * K)).T
    between = jnp.broadcast_to(between, (2 * K, 2 * K)).T
    average = top[:K]
    variance = (top[K:] + between[:K]) * (1.0 / (PIECE * plane_size * planes))
    factor = lax.rsqrt(variance + EPS)
    for p in range(pieces + 2 * REACH):
        cut = slice(p * PIECE, (p + 1) * PIECE)
        scaled = ((full[p] - average) * factor).astype(jnp.bfloat16)
        normed[:, cut] = scaled
        wide = scaled.astype(jnp.float32)
        square = jnp.sum(wide * wide, axis=0, keepdims=True)
        weight[:, cut] = 1.0 / (square * (1.0 / K) + EPS)

    for b in range(pieces):
        rows = normed[:, (b + REACH) * PIECE : (b + REACH + 1) * PIECE]
        span = slice(b * PIECE, (b + WINDOW) * PIECE)
        inner = lax.dot_general(
            rows, normed[:, span], (((0,), (0,)), ((), ())), preferred_element_type=jnp.float32
        )
        terms = inner * inner * masks[b] * weight[:, span]
        summed = terms[:, :PIECE]
        for t in range(1, WINDOW):
            summed = summed + terms[:, t * PIECE : (t + 1) * PIECE]
        line = jnp.sum(summed.T, axis=0, keepdims=True)
        own = weight[:, (b + REACH) * PIECE : (b + REACH + 1) * PIECE]
        out[b : b + 1, :] = line * own * scale[b : b + 1, :]

    wait_for(part.at[pl.ds(0, pieces - 1)], part_send)
    wait_for(full.at[pl.ds(0, pieces - 1)], full_send)
    wait_for(near.at[pl.ds(0, plane_size - 1)], near_send)
    wait_for(far.at[pl.ds(0, planes - 1)], far_send)
    low_halo.wait_send()
    high_halo.wait_send()


def on_device(packed_panel, components, bounds, band_width):
    haps, snps = lax.axis_size("hap"), lax.axis_size("snp")
    words, columns = packed_panel.shape
    pieces = columns // PIECE
    depth = -(-words * BITS // PIECE) * PIECE
    plane_size, planes = haps * PLANE, snps // PLANE
    extended = pieces + 2 * REACH
    dma = pltpu.SemaphoreType.DMA
    out = pl.pallas_call(
        functools.partial(kernel, haps, snps),
        out_shape=jax.ShapeDtypeStruct((pieces, PIECE), jnp.float32),
        in_specs=[pl.BlockSpec(memory_space=pltpu.VMEM)] * 4,
        out_specs=pl.BlockSpec(memory_space=pltpu.VMEM),
        scratch_shapes=[
            pltpu.VMEM((K, depth), jnp.bfloat16),
            pltpu.VMEM((pieces, K, PIECE), jnp.float32),
            pltpu.VMEM((pieces, K, PIECE), jnp.float32),
            pltpu.VMEM((extended, K, PIECE), jnp.float32),
            pltpu.VMEM((K, extended * PIECE), jnp.bfloat16),
            pltpu.VMEM((1, extended * PIECE), jnp.float32),
            pltpu.VMEM((pieces, PIECE, WINDOW * PIECE), jnp.float32),
            pltpu.VMEM((pieces, PIECE), jnp.float32),
            pltpu.VMEM((plane_size, 1, 2 * K), jnp.float32),
            pltpu.VMEM((planes, 1, 2 * K), jnp.float32),
            dma, dma, dma, dma, dma((2,)), dma((2,)), dma, dma, dma, dma,
        ],
        compiler_params=pltpu.CompilerParams(collective_id=0, has_side_effects=True),
    )(packed_panel, components, bounds, band_width.reshape(pieces, PIECE))
    return out.reshape(columns)


def solution(mesh):
    return jax.shard_map(
        on_device,
        mesh=mesh,
        in_specs=(P("hap", "snp"), P(None, "hap"), P(None, "snp"), P("snp")),
        out_specs=P("snp"),
        check_vma=False,
    )
```

```python
import functools

import jax
import jax.numpy as jnp
from jax import lax
from jax.experimental import pallas as pl
from jax.experimental.pallas import tpu as pltpu
from jax.sharding import PartitionSpec as P

EPS = 1e-06
K = 64
BITS = 13
PIECE = 128
REACH = 2
WINDOW = 2 * REACH + 1
PLANE = 4
MESH = pl.DeviceIdType.MESH


def ring(value, size):
    return lax.rem(value, size)


def kernel(
    haps, snps, panel_in, comp_in, bounds_in, width_in, out,
    panel, comp, bounds, width, comp_pad, part, recv, full, normed, weight, masks, scale, near, far,
    part_send, part_recv, full_send, full_recv, halo_send, halo_recv,
    near_send, near_recv, far_send, far_recv, panel_sem, input_sem, ready,
):
    h, s = lax.axis_index("hap"), lax.axis_index("snp")
    z, sub = lax.div(s, PLANE), lax.rem(s, PLANE)
    planes, plane_size = snps // PLANE, haps * PLANE
    me = h * PLANE + sub
    words, columns = panel.shape
    pieces = columns // PIECE
    left, right = ring(s + snps - 1, snps), ring(s + 1, snps)

    def in_plane(r):
        q = ring(me + r, plane_size)
        return (lax.div(q, PLANE), z * PLANE + lax.rem(q, PLANE))

    def along_z(r):
        return (h, ring(z + r, planes) * PLANE + sub)

    blocks = pieces // 2
    mine, side = lax.div(h, 2), lax.rem(h, 2)
    order = sorted(range(blocks), key=lambda d: (-min(d, blocks - d), d))

    def fetch(turn):
        at = pl.multiple_of(ring(mine + order[turn], blocks) * (2 * PIECE), 2 * PIECE)
        cut = pl.ds(at, 2 * PIECE)
        return pltpu.make_async_copy(panel_in.at[:, cut], panel.at[:, cut], panel_sem.at[turn])

    inputs = [
        pltpu.make_async_copy(comp_in, comp, input_sem.at[0]),
        pltpu.make_async_copy(bounds_in, bounds, input_sem.at[1]),
        pltpu.make_async_copy(width_in, width, input_sem.at[2]),
    ]
    inputs[0].start()
    for turn in range(blocks):
        fetch(turn).start()
    inputs[1].start()
    inputs[2].start()

    barrier = pltpu.get_barrier_semaphore()

    def signal(sem, device):
        pl.semaphore_signal(sem, inc=1, device_id=device, device_id_type=MESH)

    for r in range(1, haps):
        signal(barrier, (ring(h + r, haps), s))
    for r in range(1, PLANE):
        signal(barrier, (h, z * PLANE + ring(sub + r, PLANE)))
    signal(barrier, along_z(1))
    signal(barrier, along_z(planes - 1))

    depth = comp_pad.shape[1]
    col = lax.broadcasted_iota(jnp.int32, (8, depth), 1)
    bit = jnp.zeros_like(col)
    for j in range(1, BITS + 1):
        bit = bit + (col >= j * words).astype(jnp.int32)
    source = jnp.where(col < words * BITS, BITS * (col - words * bit) + bit, -1)[:1]
    level = (jnp.right_shift(1 << (BITS - 1), bit).astype(jnp.float32) * (0.5 ** (BITS - 1)))[:1]
    row = lax.broadcasted_iota(jnp.int32, (depth, depth), 0)
    chosen = jnp.where(row == source, level, 0.0).astype(jnp.bfloat16)
    comp_pad[...] = jnp.zeros_like(comp_pad)
    inputs[0].wait()
    comp_pad[:, : comp.shape[1]] = comp[...]
    mixed = jnp.dot(comp_pad[...], chosen, preferred_element_type=jnp.float32).astype(jnp.bfloat16)

    def project(block):
        at = pl.multiple_of(block * (2 * PIECE), 2 * PIECE)
        packed = panel[:, pl.ds(at, 2 * PIECE)]
        alleles = [
            jnp.bitwise_and(packed, 1 << j).astype(jnp.float32).astype(jnp.bfloat16)
            for j in range(BITS)
        ]
        rest = depth - BITS * words
        alleles.append(jnp.zeros((rest, 2 * PIECE), jnp.bfloat16))
        product = jnp.dot(
            mixed, jnp.concatenate(alleles, axis=0), preferred_element_type=jnp.float32
        )
        part[2 * block] = product[:, :PIECE]
        part[2 * block + 1] = product[:, PIECE:]

    def send_part(to):
        return pltpu.make_async_remote_copy(
            part.at[to], recv.at[h], part_send, part_recv, device_id=(to, s), device_id_type=MESH
        )

    rounds = [1 << k for k in range(8) if (2 << k) <= planes // 2]

    def tell(k):
        if k < len(rounds):
            signal(ready.at[k], along_z(rounds[k]))
            signal(ready.at[k], along_z(planes - rounds[k]))

    def hear(k):
        if k < len(rounds):
            pl.semaphore_wait(ready.at[k], 2)

    for turn, d in enumerate(order):
        block = ring(mine + d, blocks)
        fetch(turn).wait()
        project(block)
        if turn == 0:
            pl.semaphore_wait(barrier, haps + PLANE)
            tell(0)
        if d:
            send_part(2 * block + side).start()
            send_part(2 * block + 1 - side).start()
        else:
            send_part(2 * block + 1 - side).start()
    recv[h] = part[h]
    hear(0)
    tell(1)

    def wait_for(ref, sem):
        pltpu.make_async_copy(ref, ref, sem).wait()

    wait_for(recv.at[pl.ds(0, pieces - 1)], part_recv)
    total = recv[0]
    for k in range(1, pieces):
        total = total + recv[k]
    full[REACH + h] = total

    lane = lax.broadcasted_iota(jnp.int32, (1, 2 * K), 1)
    first = lane < K
    both = jnp.concatenate([total, total], axis=0).T
    average = jnp.sum(both, axis=0, keepdims=True) * (1.0 / PIECE)
    off = both - average
    spread = jnp.sum(off * off, axis=0, keepdims=True)
    near[me] = jnp.where(first, average, spread)

    def send_near(r):
        return pltpu.make_async_remote_copy(
            near.at[me], near.at[me], near_send, near_recv,
            device_id=in_plane(r), device_id_type=MESH,
        )

    @pl.loop(1, plane_size)
    def _(r):
        send_near(r).start()

    def send_full(r):
        to = ring(h + r, haps)
        return pltpu.make_async_remote_copy(
            full.at[REACH + h], full.at[REACH + h], full_send, full_recv,
            device_id=(to, s), device_id_type=MESH,
        )

    for r in range(1, haps):
        send_full(r).start()

    hear(1)
    tell(2)

    def merge(ref, count, weight_each):
        rows = [ref[k] for k in range(count)]
        summed = functools.reduce(jnp.add, rows)
        mean = summed * (1.0 / count)
        offs = [r - mean for r in rows]
        between = functools.reduce(jnp.add, [o * o for o in offs]) * weight_each
        return mean, summed, between

    position = lax.broadcasted_iota(jnp.int32, (1, PIECE), 1)
    lane_at = lax.broadcasted_iota(jnp.int32, (PIECE, PIECE), 1)
    row_at = lax.broadcasted_iota(jnp.int32, (PIECE, PIECE), 0)

    def windows(b):
        at = s * columns + b * PIECE
        here = position + at
        reach = width[b : b + 1, :]
        cut = slice(b * PIECE, (b + 1) * PIECE)
        low = jnp.maximum(bounds[0:1, cut], here - reach)
        high = jnp.minimum(bounds[1:2, cut], here + reach)
        count = (high - low).astype(jnp.float32)
        scale[b : b + 1, :] = (1.0 / K) / jnp.maximum(count, 1.0)
        start = at - REACH * PIECE
        low_rows = jnp.broadcast_to((low - start).astype(jnp.float32), (PIECE, PIECE)).T
        high_rows = jnp.broadcast_to((high - start).astype(jnp.float32), (PIECE, PIECE)).T
        for t in range(WINDOW):
            there = (lane_at + t * PIECE).astype(jnp.float32)
            inside = (there >= low_rows) & (there <= high_rows)
            if t == REACH:
                inside = inside & (lane_at != row_at)
            masks[b, :, t * PIECE : (t + 1) * PIECE] = inside.astype(jnp.float32)

    inputs[1].wait()
    inputs[2].wait()
    for b in range(pieces):
        windows(b)

    wait_for(near.at[pl.ds(0, plane_size - 1)], near_recv)
    mean, summed, between = merge(near, plane_size, float(PIECE))
    moved = pltpu.roll(jnp.broadcast_to(between, (8, 2 * K)), K, 1)[:1]
    far[z] = jnp.where(first, mean, summed + moved)

    def send_far(r):
        return pltpu.make_async_remote_copy(
            far.at[z], far.at[z], far_send, far_recv, device_id=along_z(r), device_id_type=MESH
        )

    hear(2)
    @pl.loop(1, planes)
    def _(r):
        send_far(r).start()

    wait_for(full.at[pl.ds(REACH, haps - 1)], full_recv)
    low_halo = pltpu.make_async_remote_copy(
        full.at[pl.ds(pieces, REACH)], full.at[pl.ds(0, REACH)],
        halo_send.at[0], halo_recv.at[0], device_id=(h, right), device_id_type=MESH,
    )
    high_halo = pltpu.make_async_remote_copy(
        full.at[pl.ds(REACH, REACH)], full.at[pl.ds(REACH + pieces, REACH)],
        halo_send.at[1], halo_recv.at[1], device_id=(h, left), device_id_type=MESH,
    )
    low_halo.start()
    high_halo.start()
    low_halo.wait_recv()
    high_halo.wait_recv()

    wait_for(far.at[pl.ds(0, planes - 1)], far_recv)
    mean, summed, between = merge(far, planes, float(PIECE * plane_size))
    top = jnp.broadcast_to(jnp.where(first, mean, summed), (2 * K, 2 * K)).T
    between = jnp.broadcast_to(between, (2 * K, 2 * K)).T
    average = top[:K]
    variance = (top[K:] + between[:K]) * (1.0 / (PIECE * plane_size * planes))
    factor = lax.rsqrt(variance + EPS)
    for p in range(pieces + 2 * REACH):
        cut = slice(p * PIECE, (p + 1) * PIECE)
        scaled = ((full[p] - average) * factor).astype(jnp.bfloat16)
        normed[:, cut] = scaled
        wide = scaled.astype(jnp.float32)
        square = jnp.sum(wide * wide, axis=0, keepdims=True)
        weight[:, cut] = 1.0 / (square * (1.0 / K) + EPS)

    for b in range(pieces):
        rows = normed[:, (b + REACH) * PIECE : (b + REACH + 1) * PIECE]
        span = slice(b * PIECE, (b + WINDOW) * PIECE)
        inner = lax.dot_general(
            rows, normed[:, span], (((0,), (0,)), ((), ())), preferred_element_type=jnp.float32
        )
        terms = inner * inner * masks[b] * weight[:, span]
        summed = terms[:, :PIECE]
        for t in range(1, WINDOW):
            summed = summed + terms[:, t * PIECE : (t + 1) * PIECE]
        line = jnp.sum(summed.T, axis=0, keepdims=True)
        own = weight[:, (b + REACH) * PIECE : (b + REACH + 1) * PIECE]
        out[b : b + 1, :] = line * own * scale[b : b + 1, :]

    wait_for(part.at[pl.ds(0, pieces - 1)], part_send)
    wait_for(full.at[pl.ds(0, pieces - 1)], full_send)
    wait_for(near.at[pl.ds(0, plane_size - 1)], near_send)
    wait_for(far.at[pl.ds(0, planes - 1)], far_send)
    low_halo.wait_send()
    high_halo.wait_send()


def on_device(packed_panel, components, bounds, band_width):
    haps, snps = lax.axis_size("hap"), lax.axis_size("snp")
    words, columns = packed_panel.shape
    pieces = columns // PIECE
    depth = -(-words * BITS // PIECE) * PIECE
    plane_size, planes = haps * PLANE, snps // PLANE
    extended = pieces + 2 * REACH
    dma = pltpu.SemaphoreType.DMA
    out = pl.pallas_call(
        functools.partial(kernel, haps, snps),
        out_shape=jax.ShapeDtypeStruct((pieces, PIECE), jnp.float32),
        in_specs=[pl.BlockSpec(memory_space=pltpu.HBM)] * 4,
        out_specs=pl.BlockSpec(memory_space=pltpu.VMEM),
        scratch_shapes=[
            pltpu.VMEM((words, columns), jnp.int32),
            pltpu.VMEM((K, words * BITS), jnp.bfloat16),
            pltpu.VMEM((2, columns), jnp.int32),
            pltpu.VMEM((pieces, PIECE), jnp.int32),
            pltpu.VMEM((K, depth), jnp.bfloat16),
            pltpu.VMEM((pieces, K, PIECE), jnp.float32),
            pltpu.VMEM((pieces, K, PIECE), jnp.float32),
            pltpu.VMEM((extended, K, PIECE), jnp.float32),
            pltpu.VMEM((K, extended * PIECE), jnp.bfloat16),
            pltpu.VMEM((1, extended * PIECE), jnp.float32),
            pltpu.VMEM((pieces, PIECE, WINDOW * PIECE), jnp.float32),
            pltpu.VMEM((pieces, PIECE), jnp.float32),
            pltpu.VMEM((plane_size, 1, 2 * K), jnp.float32),
            pltpu.VMEM((planes, 1, 2 * K), jnp.float32),
            dma, dma, dma, dma, dma((2,)), dma((2,)), dma, dma, dma, dma,
            dma((pieces // 2,)), dma((3,)), pltpu.SemaphoreType.REGULAR((3,)),
        ],
        compiler_params=pltpu.CompilerParams(collective_id=0, has_side_effects=True),
    )(packed_panel, components, bounds, band_width.reshape(pieces, PIECE))
    return out.reshape(columns)


def solution(mesh):
    return jax.shard_map(
        on_device,
        mesh=mesh,
        in_specs=(P("hap", "snp"), P(None, "hap"), P(None, "snp"), P("snp")),
        out_specs=P("snp"),
        check_vma=False,
    )
```
